32 devices in a mesh: rep: 1 (over z), r: 4 (over y), s: 8 (over x, core).
Axes of the slice: x: 4, y: 4, z: 1, core: 2. Of those that a mesh axis runs over, the one named last changes fastest.
The devices are a block of a 4x4x8 slice.
Arguments:
- x: bfloat16 [32, 4096, 512], P(('rep', 'r', 's'))
- dy: bfloat16 [32, 4096, 512], P(('rep', 'r', 's'))
- w_gate: bfloat16 [2, 512, 2048], P(None, 's')
- w_up: bfloat16 [2, 512, 2048], P(None, 's')
- w_down: bfloat16 [2, 2048, 512], P(None, 's')
Outputs:
- output 1: bfloat16 [32, 4096, 512], P(('rep', 'r', 's'))
- output 2: bfloat16 [2, 512, 2048], P('rep', 's')
- output 3: bfloat16 [2, 512, 2048], P('rep', 's')
- output 4: bfloat16 [2, 2048, 512], P('rep', 's')
All inputs are finite; a program needn't handle non-finite values.
Results may differ from the reference program's by a relative error of at most 0.018.
Values are sent between devices in bfloat16 or wider.
A program may use at most 768 MiB of HBM per device.

```python
import jax
import jax.numpy as jnp
from jax import lax

SEQUENCES = 32
TOKENS = 4096
D = 512
FF = 2048
LAYERS = 2
NAMES = ("w_gate", "w_up", "w_down")
SHAPES = {"w_gate": (LAYERS, D, FF), "w_up": (LAYERS, D, FF), "w_down": (LAYERS, FF, D)}


def bump(key, n, height):
    away = (jnp.arange(n, dtype=jnp.int32) - jax.random.randint(key, (), 0, n, jnp.int32)) % n
    return jnp.where(away < n // 8, height, 1.0)


def together(key, own, strength):
    shared = jax.random.normal(key, own.shape[1:], jnp.float32)
    return (own + strength * shared) * lax.rsqrt(1 + strength * strength)


def setup_inputs(seed: int = 0, part: int = 0) -> dict:
    kx, kdy, ka, kb, kz, kf, kh, kl, *kw = jax.random.split(jax.random.key(seed), 8 + len(NAMES))
    kx, kdy, ka, kb = (jax.random.fold_in(k, part) for k in (kx, kdy, ka, kb))
    shape = (SEQUENCES, TOKENS, D)
    much_x, much_dy = jax.random.uniform(kz, (2,), jnp.float32, 0.0, 1.0)
    layers = 2.0 ** jax.random.uniform(kl, (LAYERS, 1, 1), jnp.float32, -1.0, 1.0)
    x = together(ka, jax.random.normal(kx, shape, jnp.float32), much_x) * bump(kf, D, 4.0)
    dy = together(kb, jax.random.normal(kdy, shape, jnp.float32), much_dy)
    drawn = {"x": x.astype(jnp.bfloat16), "dy": (dy * (SEQUENCES * TOKENS) ** -0.5).astype(jnp.bfloat16)}
    for key, name in zip(kw, NAMES, strict=True):
        w = jax.random.normal(key, SHAPES[name], jnp.float32) * SHAPES[name][1] ** -0.5
        drawn[name] = (w * {"w_gate": 1.0, "w_up": bump(kh, FF, 4.0), "w_down": layers}[name]).astype(jnp.bfloat16)
    return drawn


def matmul(a, w):
    return jnp.dot(a, w, preferred_element_type=jnp.float32).astype(jnp.bfloat16)


def normed(h):
    wide = h.astype(jnp.float32)
    scale = lax.rsqrt(jnp.mean(wide**2, -1, keepdims=True) + 1e-6)
    return (wide * scale).astype(jnp.bfloat16)


def layer(h, w):
    a = normed(h)
    gate = jnp.dot(a, w["w_gate"], preferred_element_type=jnp.float32)
    up = jnp.dot(a, w["w_up"], preferred_element_type=jnp.float32)
    return h + matmul((jax.nn.silu(gate) * up).astype(jnp.bfloat16), w["w_down"])


def stack(weights, h):
    return lax.scan(lambda h, w: (layer(h, w), None), h, weights)[0]


def reference(x, dy, w_gate, w_up, w_down):
    weights = dict(zip(NAMES, (w_gate, w_up, w_down), strict=True))

    def take(so_far, sequence):
        h, by_y = sequence
        _, back = jax.vjp(stack, weights, h)
        by_weights, by_h = back(by_y)
        return jax.tree.map(lambda total, term: total + term.astype(jnp.float32), so_far, by_weights), by_h

    none_yet = {name: jnp.zeros(w.shape, jnp.float32) for name, w in weights.items()}
    by_weights, by_x = lax.scan(take, none_yet, (x, dy))
    return (by_x, *(by_weights[name].astype(jnp.bfloat16) for name in NAMES))
```

```python
import functools

import jax
import jax.numpy as jnp
from jax import lax
from jax.experimental import pallas as pl
from jax.experimental.pallas import tpu as pltpu
from jax.sharding import PartitionSpec as P

F32, BF16 = jnp.float32, jnp.bfloat16
NN = (((1,), (0,)), ((), ()))
NT = (((1,), (1,)), ((), ()))
TN = (((0,), (0,)), ((), ()))
CHUNKS = 4
TILES = 4


def dot(a, b, dims=NN):
    return lax.dot_general(a, b, dims, preferred_element_type=F32)


def inverse(wide):
    return lax.rsqrt(jnp.mean(wide * wide, -1, keepdims=True) + 1e-6)


def sigmoid(x):
    return 0.5 * jnp.tanh(0.5 * x) + 0.5


def kernel(nx, ny, layers, x_hbm, dy_hbm, wg_hbm, wu_hbm, wd_hbm, dx_hbm, og, ou, od,
           wa, wd, act_in, h, g, total, acc, ds, dr, x1s, x1r, x2s, x2r, pf, pb, yr, fb, eb,
           load_sem, w_sem, ag_send, ag_recv, d_send, d_recv, x1_send, x1_recv, x2_send, x2_recv,
           y1_send, y1_recv, y2_send, y2_recv, e_send, e_recv):
    place = lax.axis_index("s")
    y = lax.axis_index("r")
    i, c = place // 2, place % 2
    right, left, across = (i + 1) % nx, (i + nx - 1) % nx, (i + 2) % nx
    partner = {"s": 2 * i + 1 - c}
    to_right, to_left = {"s": 2 * right + c}, {"s": 2 * left + c}
    rows_y = [(y + d) % ny for d in range(1, ny)]
    tokens, width = h.shape
    tile = tokens // TILES
    piece = wa.shape[-2]
    half = piece // 2
    lanes = 128
    steps = layers * CHUNKS

    def rows(t):
        return pl.ds(pl.multiple_of(t * tile, tile), tile)

    def remote(src, dst, send, recv, device):
        return pltpu.make_async_remote_copy(src_ref=src, dst_ref=dst, send_sem=send, recv_sem=recv,
                                            device_id=device, device_id_type=pl.DeviceIdType.MESH)

    items = []
    for l in range(layers):
        for k in range(CHUNKS // 2):
            items += [("a", l, 2 * k), ("b", l, k), ("a", l, 2 * k + 1)]

    def block(item, owner, part=None):
        kind, l, f = item
        if kind == "a":
            ref = wa.at[l * CHUNKS + f]
            return ref.at[:, owner, c] if part is None else ref.at[part, owner, c]
        ref = wd.at[l * CHUNKS + 2 * f + c]
        return ref.at[owner] if part is None else ref.at[owner, pl.ds(part * piece, piece)]

    def whole(item):
        kind, l, f = item
        return wa.at[l * CHUNKS + f, :, :, c] if kind == "a" else wd.at[l * CHUNKS + 2 * f + c]

    def own_copies(n):
        kind, l, f = items[n]
        if kind == "b":
            return [pltpu.make_async_copy(wd_hbm.at[l, pl.ds(f * lanes, lanes)], block(items[n], i), w_sem.at[n])]
        k, cc = f // 2, f % 2
        return [
            pltpu.make_async_copy(
                w_hbm.at[l, :, pl.ds((2 * ii + cc) * 2 * lanes + k * lanes, lanes)],
                wa.at[l * CHUNKS + f, m, i, c, :, pl.ds(ii * lanes, lanes)],
                w_sem.at[n],
            )
            for m, w_hbm in enumerate((wg_hbm, wu_hbm))
            for ii in range(nx)
        ]

    def own_wait(n):
        ref = block(items[n], i)
        pltpu.make_async_copy(ref, ref, w_sem.at[n]).wait()

    def ring(n):
        it = items[n]
        return (
            remote(block(it, i), block(it, i), ag_send.at[n, 0], ag_recv.at[n, 0], to_right),
            remote(block(it, i), block(it, i), ag_send.at[n, 1], ag_recv.at[n, 1], to_left),
        )

    def ring_in(n):
        it = items[n]
        return (
            remote(block(it, left), block(it, left), ag_send.at[n, 0], ag_recv.at[n, 0], to_right),
            remote(block(it, right), block(it, right), ag_send.at[n, 1], ag_recv.at[n, 1], to_left),
        )

    def relay(n):
        it = items[n]
        return (
            remote(block(it, left, 0), block(it, left, 0), ag_send.at[n, 2], ag_recv.at[n, 2], to_right),
            remote(block(it, right, 1), block(it, right, 1), ag_send.at[n, 3], ag_recv.at[n, 3], to_left),
        )

    def relay_in(n):
        it = items[n]
        return (
            remote(block(it, across, 0), block(it, across, 0), ag_send.at[n, 2], ag_recv.at[n, 2], to_right),
            remote(block(it, across, 1), block(it, across, 1), ag_send.at[n, 3], ag_recv.at[n, 3], to_left),
        )

    def cross(n):
        return remote(whole(items[n]), whole(items[n]), ag_send.at[n, 4], ag_recv.at[n, 4], partner)

    def cross_in(n):
        kind, l, f = items[n]
        ref = wa.at[l * CHUNKS + f, :, :, 1 - c] if kind == "a" else wd.at[l * CHUNKS + 2 * f + 1 - c]
        return remote(ref, ref, ag_send.at[n, 4], ag_recv.at[n, 4], partner)

    def s0(n):
        own_wait(n)
        for copy in ring(n):
            copy.start()

    def s1(n):
        for copy in ring_in(n):
            copy.wait_recv()
        for copy in relay(n):
            copy.start()

    def s2(n):
        for copy in relay_in(n):
            copy.wait_recv()
        for copy in ring(n):
            copy.wait_send()
        for copy in relay(n):
            copy.wait_send()
        cross(n).start()

    def s3(n):
        cross_in(n).wait_recv()
        cross(n).wait_send()

    def z(par, j, part=None):
        start, count = (0, piece) if part is None else (part * half, half)
        mine = acc[par, :, pl.ds(pl.multiple_of(j * 2 * piece + c * piece + start, half), count), :]
        return mine + dr[par, j, :, pl.ds(start, count), :].astype(F32)

    def d_copy(par):
        return remote(ds, dr.at[par], d_send.at[par], d_recv.at[par], partner)

    def x1_copies(par):
        return (remote(x1s.at[0], x1r.at[par, 0], x1_send.at[0], x1_recv.at[par, 0], to_right),
                remote(x1s.at[1], x1r.at[par, 1], x1_send.at[1], x1_recv.at[par, 1], to_left))

    def x2_copies():
        return (remote(x2s.at[0], x2r.at[0], x2_send.at[0], x2_recv.at[0], to_right),
                remote(x2s.at[1], x2r.at[1], x2_send.at[1], x2_recv.at[1], to_left))

    def y1_copies():
        return [remote(pb.at[to], yr.at[d], y1_send.at[d], y1_recv.at[d], {"r": to}) for d, to in enumerate(rows_y)]

    def y2_copies():
        return [remote(fb.at[y], fb.at[y], y2_send.at[d], y2_recv.at[d], {"r": to}) for d, to in enumerate(rows_y)]

    def y2_in():
        return [
            remote(fb.at[(y + ny - d) % ny], fb.at[(y + ny - d) % ny], y2_send.at[d - 1], y2_recv.at[d - 1],
                   {"r": rows_y[d - 1]})
            for d in range(1, ny)
        ]

    def e_copy(par):
        return remote(fb.at[:, 2], eb.at[par], e_send.at[par], e_recv.at[par], partner)

    def stage0(q):
        par = q % 2
        for j in range(nx):
            ds[j] = acc[par, :, pl.ds(pl.multiple_of(j * 2 * piece + (1 - c) * piece, piece), piece), :].astype(BF16)
        d_copy(par).start()

    def stage1(q):
        par = q % 2
        d_copy(par).wait()
        x1s[0, 0] = z(par, across, 0).astype(BF16)
        x1s[0, 1] = z(par, right, 1).astype(BF16)
        x1s[1, 0] = z(par, across, 1).astype(BF16)
        x1s[1, 1] = z(par, left, 0).astype(BF16)
        for copy in x1_copies(par):
            copy.start()

    def stage2(q):
        par = q % 2
        for copy in x1_copies(par):
            copy.wait()
        x2s[0] = (z(par, right, 0) + x1r[par, 0, 0].astype(F32)).astype(BF16)
        x2s[1] = (z(par, left, 1) + x1r[par, 1, 0].astype(F32)).astype(BF16)
        for copy in x2_copies():
            copy.start()

    def stage3(q):
        par = q % 2
        for copy in x2_copies():
            copy.wait()
        pf[:, :half] = z(par, i, 0) + x2r[0].astype(F32) + x1r[par, 1, 1].astype(F32)
        pf[:, half:] = z(par, i, 1) + x2r[1].astype(F32) + x1r[par, 0, 1].astype(F32)
        part = piece // ny
        for to in range(ny):
            pb[to] = pf[:, to * part:(to + 1) * part].astype(BF16)
        for copy in y1_copies():
            copy.start()

    def stage4(q):
        for copy in y1_copies():
            copy.wait()
        part = piece // ny
        mine = pf[:, pl.ds(pl.multiple_of(y * part, part), part), :]
        for d in range(ny - 1):
            mine = mine + yr[d].astype(F32)
        fb[y] = mine.astype(BF16)
        for copy in y2_copies():
            copy.start()

    def stage5(q):
        for copy in y2_in():
            copy.wait_recv()
        for copy in y2_copies():
            copy.wait_send()
        e_copy(q % 2).start()

    def stage6(q):
        par = q % 2
        e_copy(par).wait()
        l, f = layers - 1 - q // CHUNKS, q % CHUNKS
        k, cc = f // 2, f % 2
        for m, out in ((0, og), (1, ou)):
            for ii in range(nx):
                cols = pl.ds(pl.multiple_of((2 * ii + cc) * 2 * lanes + k * lanes, lanes), lanes)
                out[l, :, cols] = fb[:, m, :, ii * lanes:(ii + 1) * lanes].reshape(piece, lanes)

        @pl.when(c == cc)
        def _():
            od[l, pl.ds(pl.multiple_of(k * lanes + c * piece, piece), piece), :] = fb[:, 2].reshape(piece, width)
            od[l, pl.ds(pl.multiple_of(k * lanes + (1 - c) * piece, piece), piece), :] = eb[par].reshape(piece, width)

    x_in = pltpu.make_async_copy(x_hbm.at[0], h, load_sem.at[0])
    dy_in = pltpu.make_async_copy(dy_hbm.at[0], g, load_sem.at[1])
    for copy in own_copies(0) + own_copies(1):
        copy.start()
    x_in.start()
    for n in range(2, len(items)):
        for copy in own_copies(n):
            copy.start()
    dy_in.start()
    barrier = pltpu.get_barrier_semaphore()
    peers = [partner, to_right, to_left] + [{"r": to} for to in rows_y]
    for device in peers:
        pl.semaphore_signal(barrier, inc=1, device_id=device, device_id_type=pl.DeviceIdType.MESH)
    pl.semaphore_wait(barrier, len(peers))
    s0(0)
    s0(1)
    x_in.wait()

    def first_norm(t, _):
        wide = h[rows(t), :].astype(F32)
        act_in[0, rows(t), :] = (wide * inverse(wide)).astype(BF16)
        return 0

    lax.fori_loop(0, TILES, first_norm, 0)
    s1(0)
    s0(2)
    s1(1)
    s2(0)
    s0(3)
    s2(1)
    s3(0)
    s3(1)

    def matrix(ref):
        return ref.reshape(-1, ref.shape[-1])

    sent = 2
    for l in range(layers - 1):
        for f in range(CHUNKS):
            lf = l * CHUNKS + f

            def forward(t):
                r = rows(t)
                a = act_in[l, r, :]
                gate = dot(a, matrix(wa[lf, 0]))
                up = dot(a, matrix(wa[lf, 1]))
                hidden = (gate * sigmoid(gate) * up).astype(BF16)
                down = dot(hidden, matrix(wd[lf]))
                if f > 0:
                    down = total[r, :] + down
                if f < CHUNKS - 1:
                    total[r, :] = down
                else:
                    new = h[r, :] + down.astype(BF16)
                    h[r, :] = new
                    wide = new.astype(F32)
                    act_in[l + 1, r, :] = (wide * inverse(wide)).astype(BF16)
                    total[r, :] = jnp.zeros((tile, width), F32)

            def pair(p, _, n0=sent):
                forward(2 * p)
                for u in range(2):
                    @pl.when(p == u)
                    def _(n=n0 + u):
                        s1(n)
                        s0(n + 2)
                forward(2 * p + 1)
                for u in range(2):
                    @pl.when(p == u)
                    def _(n=n0 + u):
                        s2(n)
                return 0

            lax.fori_loop(0, TILES // 2, pair, 0)
            sent += 2
            for n in ((2,), (3, 4), (5,), (6, 7))[f]:
                s3(n)

    dy_in.wait()

    def norm_back(t):
        r = rows(t)
        wide = h[r, :].astype(F32)
        scale = inverse(wide)
        n = wide * scale
        dn = total[r, :].astype(BF16).astype(F32)
        dh = scale * (dn - n * jnp.mean(n * dn, -1, keepdims=True))
        g[r, :] = g[r, :] + dh.astype(BF16)

    def chunk(q, _):
        par, l, f = q % 2, layers - 1 - q // CHUNKS, q % CHUNKS
        lf = l * CHUNKS + f
        for m in range(3):
            acc[par, m] = jnp.zeros(acc.shape[2:], F32)

        def step(t, _):
            r = rows(t)
            a, dh = act_in[l, r, :], g[r, :]
            gate = dot(a, matrix(wa[lf, 0]))
            up = dot(a, matrix(wa[lf, 1]))
            dact = dot(dh, matrix(wd[lf]), NT).astype(BF16).astype(F32)
            s = sigmoid(gate)
            sg = gate * s
            hidden = (sg * up).astype(BF16)
            dup = (dact * sg).astype(BF16)
            dgate = (dact * up * (s + sg * (1 - s))).astype(BF16)
            acc[par, 0] += dot(a, dgate, TN)
            acc[par, 1] += dot(a, dup, TN)
            acc[par, 2] += dot(hidden, dh, TN)
            total[r, :] += dot(dgate, matrix(wa[lf, 0]), NT) + dot(dup, matrix(wa[lf, 1]), NT)

            @pl.when((q >= 1) & (t == 0))
            def _():
                stage1(q - 1)

            @pl.when((q >= 2) & (t == 0))
            def _():
                stage5(q - 2)

            @pl.when((q >= 1) & (t == 1))
            def _():
                stage2(q - 1)

            @pl.when((q >= 2) & (t == 1))
            def _():
                stage6(q - 2)

            @pl.when((q >= 1) & (t == 2))
            def _():
                stage3(q - 1)

            @pl.when((q >= 1) & (t == 3))
            def _():
                stage4(q - 1)

            for u, (work, n) in enumerate(((s1, 10), (s2, 10), (s1, 11), (s2, 11))):
                @pl.when((q == 0) & (t == u))
                def _(work=work, n=n):
                    work(n)
            return 0

        lax.fori_loop(0, TILES, step, 0)
        stage0(q)
        for u, ns in enumerate(((8,), (9, 10), (11,))):
            @pl.when(q == u)
            def _(ns=ns):
                for n in ns:
                    s3(n)

        @pl.when((f == CHUNKS - 1) & (l > 0))
        def _():
            def back(t, _):
                norm_back(t)
                total[rows(t), :] = jnp.zeros((tile, width), F32)
                return 0

            lax.fori_loop(0, TILES, back, 0)
            again = pltpu.make_async_copy(x_hbm.at[0], h, load_sem.at[0])
            again.start()
            again.wait()
        return 0

    lax.fori_loop(0, steps, chunk, 0)
    last = steps - 1
    stages = (lambda: (stage1(last), stage5(last - 1)), lambda: (stage2(last), stage6(last - 1)),
              lambda: stage3(last), lambda: stage4(last))
    for t, run in enumerate(stages):
        norm_back(t)
        pltpu.make_async_copy(g.at[rows(t)], dx_hbm.at[0, rows(t)], load_sem.at[t]).start()
        run()
    stage5(last)
    for t in range(TILES):
        pltpu.make_async_copy(g.at[rows(t)], dx_hbm.at[0, rows(t)], load_sem.at[t]).wait()
    stage6(last)


def solution(mesh):
    nx, ny = mesh.shape["s"] // 2, mesh.shape["r"]

    def step(x, dy, w_gate, w_up, w_down):
        layers, piece, hidden = w_gate.shape
        tokens, width = x.shape[1:]
        cut = hidden // CHUNKS
        items = layers * (CHUNKS + CHUNKS // 2)
        anywhere, vmem = pl.BlockSpec(memory_space=pl.ANY), pl.BlockSpec(memory_space=pltpu.VMEM)
        dma = pltpu.SemaphoreType.DMA
        return pl.pallas_call(
            functools.partial(kernel, nx, ny, layers),
            name="stack",
            out_shape=[jax.ShapeDtypeStruct(a.shape, a.dtype) for a in (x, w_gate, w_up, w_down)],
            in_specs=[anywhere] * 5,
            out_specs=[anywhere] + [vmem] * 3,
            scratch_shapes=[
                pltpu.VMEM((layers * CHUNKS, 2, nx, 2, piece, cut), BF16),
                pltpu.VMEM((layers * CHUNKS, nx, 2 * piece, width), BF16),
                pltpu.VMEM((layers, tokens, width), BF16),
                pltpu.VMEM((tokens, width), BF16),
                pltpu.VMEM((tokens, width), BF16),
                pltpu.VMEM((tokens, width), F32),
                pltpu.VMEM((2, 3, width, cut), F32),
                pltpu.VMEM((nx, 3, piece, cut), BF16),
                pltpu.VMEM((2, nx, 3, piece, cut), BF16),
                pltpu.VMEM((2, 2, 3, piece // 2, cut), BF16),
                pltpu.VMEM((2, 2, 2, 3, piece // 2, cut), BF16),
                pltpu.VMEM((2, 3, piece // 2, cut), BF16),
                pltpu.VMEM((2, 3, piece // 2, cut), BF16),
                pltpu.VMEM((3, piece, cut), F32),
                pltpu.VMEM((ny, 3, piece // ny, cut), BF16),
                pltpu.VMEM((ny - 1, 3, piece // ny, cut), BF16),
                pltpu.VMEM((ny, 3, piece // ny, cut), BF16),
                pltpu.VMEM((2, ny, piece // ny, cut), BF16),
                dma((4,)),
                dma((items,)),
                dma((items, 5)),
                dma((items, 5)),
                dma((2,)), dma((2,)),
                dma((2,)), dma((2, 2)),
                dma((2,)), dma((2,)),
                dma((ny - 1,)), dma((ny - 1,)),
                dma((ny - 1,)), dma((ny - 1,)),
                dma((2,)), dma((2,)),
            ],
            compiler_params=pltpu.CompilerParams(collective_id=0, has_side_effects=True, vmem_limit_bytes=67043328),
        )(x, dy, w_gate, w_up, w_down)

    states, cut = P(("rep", "r", "s"), None, None), P(None, "s", None)
    return jax.shard_map(
        step,
        mesh=mesh,
        in_specs=(states, states) + (cut,) * 3,
        out_specs=(states,) + (P("rep", "s", None),) * 3,
        check_vma=False,
    )
```
